32 devices in a mesh: shard: 8 (over z, y), model: 4 (over x, core).
Axes of the slice: x: 2, y: 2, z: 4, core: 2. Of those that a mesh axis runs over, the one named last changes fastest.
Arguments:
- gradients: float32 [32, 128, 4096], P(None, 'shard', 'model'), may hold values from -6 to 6
- momentum: float32 [32, 128, 4096], P(None, 'shard', 'model'), may hold values from -6 to 6
- weights: float32 [32, 128, 4096], P(None, 'shard', 'model'), may hold values from -0.1875 to 0.1875
Outputs:
- new_weights: float32 [32, 128, 4096], P(None, 'shard', 'model')
- new_momentum: float32 [32, 128, 4096], P(None, 'shard', 'model')
The draws below stay inside these ranges and needn't reach their ends.
All inputs are finite; a program needn't handle non-finite values.
Results may differ from the reference program's by a relative error of at most 0.00015.
Values sent between devices are 32-bit elements; how exact they have to be, the bound alone decides.
A program may use at most 128 MiB of HBM per device.

```python
import jax
import jax.numpy as jnp
from jax import lax

SIDE = 128
WIDE = 4096
MATS = 32
ITERS = 4


def level_of(stream_key, dims, cuts, low, top_value):
    def one(position, shards_of):
        steps = jax.random.uniform(jax.random.fold_in(jax.random.fold_in(stream_key, 6), position), (shards_of,), jnp.float32, low / len(cuts), top_value / len(cuts))
        return jnp.repeat(jnp.exp(steps), dims[position] // shards_of).reshape((-1,) + (1,) * (len(dims) - position - 1))

    level = one(*cuts[0])
    for cut in cuts[1:]:
        level = level * one(*cut)
    return level


def gaussian(rng, shape, width, reach, cuts=(), held_as=jnp.bfloat16):
    result = width * jax.random.normal(rng, shape, jnp.float32)
    if cuts:
        result = result * level_of(rng, shape, cuts, -0.22, 0.18)
    return jnp.clip(result, -reach, reach).astype(held_as)


def setup_inputs(seed: int = 0) -> dict:
    key_of = jax.random.split(jax.random.key(seed), 4)
    gradients = gaussian(key_of[0], (MATS, SIDE, WIDE), 1.0, 6.0, ((1, 8), (2, 4)), jnp.float32)
    momentum = gaussian(key_of[1], (MATS, SIDE, WIDE), 1.0, 6.0, ((1, 8), (2, 4)), jnp.float32)
    weights = gaussian(key_of[2], (MATS, SIDE, WIDE), 0.03, 0.1875, ((1, 8), (2, 4)), jnp.float32)
    return {"gradients": gradients, "momentum": momentum, "weights": weights}


hold_rate = 0.8
learn_rate = 1.0

def reference(gradients, momentum, weights):
    new_momentum = hold_rate * momentum + gradients

    def orthogonal_one(stack):
        iterate = stack[None]
        iterate = iterate * lax.rsqrt(lax.optimization_barrier(jnp.sum(iterate * iterate, axis=(1, 2), keepdims=True)) + 1e-06)
        for step in range(ITERS):
            gram = jnp.einsum('mik,mjk->mij', iterate, iterate, precision=lax.Precision.HIGHEST)
            mixed = -4.775 * gram + 2.0315 * jnp.einsum('mij,mjk->mik', gram, gram, precision=lax.Precision.HIGHEST)
            iterate = 3.4445 * iterate + jnp.einsum('mij,mjk->mik', mixed, iterate, precision=lax.Precision.HIGHEST)
        return iterate[0]
    iterate = lax.map(orthogonal_one, new_momentum)
    new_weights = weights - learn_rate * iterate
    return (new_weights, new_momentum)
```

```python
import functools

import jax
import jax.numpy as jnp
from jax import lax
from jax.experimental import pallas as pl
from jax.experimental.pallas import tpu as pltpu
from jax.sharding import PartitionSpec as P

ITERS = 4
VMEM_LIMIT = 40 * 1024 * 1024
FINISH_LIMIT = 16 * 1024 * 1024
MESH = pl.DeviceIdType.MESH
HIGHEST = lax.Precision.HIGHEST


hold_rate = 0.8
learn_rate = 1.0


def mm(a, b):
    return jnp.dot(a, b, precision=HIGHEST, preferred_element_type=jnp.float32)


def direction(gram):
    side = gram.shape[-1]
    row = lax.broadcasted_iota(jnp.int32, (side, side), 0)
    col = lax.broadcasted_iota(jnp.int32, (side, side), 1)
    diagonal = row == col
    squares = jnp.sum(jnp.where(diagonal, gram, 0.0), axis=(0, 1), keepdims=True)
    scale = lax.rsqrt(squares + 1e-06)
    a = gram * scale * scale
    q = jnp.where(diagonal, jnp.broadcast_to(scale, gram.shape), 0.0)
    for step in range(ITERS):
        mixed = -4.775 * a + 2.0315 * mm(a, a)
        if step == 0:
            q_next = 3.4445 * q + mixed * scale
        else:
            q_next = 3.4445 * q + mm(mixed, q)
        if step < ITERS - 1:
            half = 3.4445 * a + mm(mixed, a)
            a = 3.4445 * half + mm(mixed, half)
        q = q_next
    return q


def partner(me, off, n):
    if n & (n - 1):
        return lax.rem(me + off, n)
    for bit in range(n.bit_length() - 1):
        if (off >> bit) & 1:
            me = me + (1 - 2 * ((me // (1 << bit)) % 2)) * (1 << bit)
    return me


def partners(me, n):
    offs = range(n - 1, 0, -1)
    if n & (n - 1) or n < 8:
        return [(off, partner(me, off, n)) for off in offs]
    high, next_high = me // (n // 2), me // (n // 4) % 2
    inner = lax.rem(high + next_high, 2)
    found = []
    for off in offs:
        if off < n // 2:
            found.append((off, partner(me, off, n)))
        else:
            other = off ^ (n // 4)
            found.append((off + inner * (other - off),
                          partner(me, off, n) + inner * (partner(me, other, n) - partner(me, off, n))))
    return found


def exchange_kernel(n, k, g_ref, m_ref, back_ref, new_ref, grad, moved, held, result, grams,
                    l_grad, l_moved, f_send, f_recv, g_send, g_recv, b_send, b_recv,
                    own_in, own_out, own_new, met, go):
    me = lax.axis_index("shard")
    col = lax.axis_index("model")
    local, _, rows, wide = held.shape
    side = n * rows
    early = n >= 8 and n & (n - 1) == 0
    middle = jnp.logical_and(me >= n // 2 - 2, me <= n // 2 + 1)
    hub = me == 0
    facing = (n - 1, n - 2)

    def chunk(j):
        return pl.ds(j * n, n)

    def load_grad(j):
        return pltpu.make_async_copy(g_ref.at[chunk(j)], grad.at[j], l_grad.at[j])

    def load_moved(j):
        return pltpu.make_async_copy(m_ref.at[chunk(j)], moved.at[j], l_moved.at[j])

    def store_new(j):
        return pltpu.make_async_copy(moved.at[j], new_ref.at[chunk(j)], own_new.at[j])

    def forward(j, off, to):
        return pltpu.make_async_remote_copy(
            src_ref=moved.at[j, to], dst_ref=held.at[j, me],
            send_sem=f_send.at[j, off], recv_sem=f_recv.at[j, off],
            device_id={"shard": to}, device_id_type=MESH)

    def share(j, off):
        return pltpu.make_async_remote_copy(
            src_ref=grams.at[j, col], dst_ref=grams.at[j, col],
            send_sem=g_send.at[j, off], recv_sem=g_recv.at[j, off],
            device_id={"model": partner(col, off, k)}, device_id_type=MESH)

    def backward(j, off, to):
        return pltpu.make_async_remote_copy(
            src_ref=result.at[j, to], dst_ref=back_ref.at[j * n + me],
            send_sem=b_send.at[j, off], recv_sem=b_recv.at[j, off],
            device_id={"shard": to}, device_id_type=MESH)

    def mine_in(j):
        return pltpu.make_async_copy(moved.at[j, me], held.at[j, me], own_in.at[j])

    def mine_out(j):
        return pltpu.make_async_copy(result.at[j, me], back_ref.at[j * n + me], own_out.at[j])

    def signal(semaphore, **to):
        pl.semaphore_signal(semaphore, inc=1, device_id=to, device_id_type=MESH)

    barrier = pltpu.get_barrier_semaphore()
    if early:
        @pl.when(middle)
        def _():
            for off in facing:
                signal(barrier, shard=partner(me, off, n))

        @pl.when(jnp.logical_not(hub))
        def _():
            signal(barrier, shard=0)

        @pl.when(hub)
        def _():
            for off in range(1, k):
                signal(barrier, model=partner(col, off, k))
            for to in range(1, n):
                if not n // 2 - 2 <= to <= n // 2 + 1:
                    signal(barrier, shard=to)
    else:
        for off in range(n - 1, 0, -1):
            signal(barrier, shard=partner(me, off, n))
        for off in range(1, k):
            signal(barrier, model=partner(col, off, k))

    @pl.loop(0, local)
    def _(j):
        load_moved(j).start()
        load_grad(j).start()

    def step(j):
        load_moved(j).wait()
        load_grad(j).wait()
        moved[j] = hold_rate * moved[j] + grad[j]

    def send_facing(j):
        @pl.when(middle)
        def _():
            for off in facing:
                forward(j, off, partner(me, off, n)).start()

    def send(j):
        for off, to in partners(me, n):
            if early:
                @pl.when(jnp.logical_not(jnp.logical_and(middle, off >= n - 2)))
                def _():
                    forward(j, off, to).start()
            else:
                forward(j, off, to).start()
        mine_in(j).start()

    step(0)
    if early:
        pl.semaphore_wait(barrier, jnp.where(hub, n + k - 2, jnp.where(middle, 2, 1)))
        send_facing(0)
    else:
        pl.semaphore_wait(barrier, n + k - 2)

    @pl.loop(1, local)
    def _(j):
        step(j)
        if early:
            send_facing(j)

    if early:
        @pl.when(hub)
        def _():
            for off in range(1, k):
                signal(met, model=partner(col, off, k))
            pl.semaphore_wait(met, k - 1)
            for to in range(n - 1, 0, -1):
                signal(go, shard=to)

        @pl.when(jnp.logical_not(hub))
        def _():
            pl.semaphore_wait(go, 1)

    @pl.loop(0, local)
    def _(j):
        send(j)

    @pl.loop(0, local)
    def _(j):
        store_new(j).start()

    @pl.loop(0, local)
    def _(j):
        for off in range(1, n):
            forward(j, off, partner(me, off, n)).wait_recv()
        mine_in(j).wait()
        x = held[j].reshape(side, wide)
        grams[j, col] = lax.dot_general(
            x, x, (((1,), (1,)), ((), ())), precision=HIGHEST, preferred_element_type=jnp.float32)
        for off in range(1, k):
            share(j, off).start()
        for off in range(1, k):
            share(j, off).wait_recv()
        gram = grams[j, 0]
        for i in range(1, k):
            gram = gram + grams[j, i]
        result[j] = mm(direction(gram), x).reshape(n, rows, wide)
        for off, to in partners(me, n):
            backward(j, off, to).start()
        mine_out(j).start()

    @pl.loop(0, local)
    def _(j):
        for off in range(1, n):
            forward(j, off, partner(me, off, n)).wait_send()
        for off in range(1, k):
            share(j, off).wait_send()
        store_new(j).wait()
        mine_out(j).wait()

    @pl.loop(0, local)
    def _(j):
        for off in range(1, n):
            backward(j, off, partner(me, off, n)).wait()


def by_kernel(n, k, gradients, momentum):
    mats, rows, wide = gradients.shape
    local = mats // n
    side = n * rows
    dma = pltpu.SemaphoreType.DMA
    whole = jax.ShapeDtypeStruct(gradients.shape, jnp.float32)
    return pl.pallas_call(
        functools.partial(exchange_kernel, n, k),
        out_shape=(whole, whole),
        in_specs=[pl.BlockSpec(memory_space=pltpu.HBM)] * 2,
        out_specs=[pl.BlockSpec(memory_space=pl.ANY)] * 2,
        scratch_shapes=[
            *[pltpu.VMEM((local, n, rows, wide), jnp.float32)] * 4,
            pltpu.VMEM((local, k, side, side), jnp.float32),
            dma((local,)), dma((local,)),
            dma((local, n)), dma((local, n)),
            dma((local, k)), dma((local, k)),
            dma((local, n)), dma((local, n)),
            dma((local,)), dma((local,)), dma((local,)),
            pltpu.SemaphoreType.REGULAR, pltpu.SemaphoreType.REGULAR,
        ],
        compiler_params=pltpu.CompilerParams(
            collective_id=0, has_side_effects=True, vmem_limit_bytes=VMEM_LIMIT),
    )(pltpu.with_memory_space_constraint(gradients, pltpu.HBM), pltpu.with_memory_space_constraint(momentum, pltpu.HBM))


def finish_kernel(pieces, back_ref, w_ref, new_ref, out_w, out_new, done, sem_w, sem_new):
    step = back_ref.shape[0] // pieces

    def part(i):
        return pl.ds(i * step, step)

    def put_new(i):
        return pltpu.make_async_copy(new_ref.at[part(i)], out_new.at[part(i)], sem_new.at[i])

    def put_w(i):
        return pltpu.make_async_copy(done.at[part(i)], out_w.at[part(i)], sem_w.at[i])

    for i in range(pieces):
        put_new(i).start()
    for i in range(pieces):
        done[part(i)] = w_ref[part(i)] - learn_rate * back_ref[part(i)]
        put_w(i).start()
    for i in range(pieces):
        put_new(i).wait()
        put_w(i).wait()


def finish(pieces, back, weights, new_momentum):
    whole = jax.ShapeDtypeStruct(back.shape, jnp.float32)
    hold = pl.BlockSpec(memory_space=pltpu.VMEM)
    leave = pl.BlockSpec(memory_space=pl.ANY)
    return pl.pallas_call(
        functools.partial(finish_kernel, pieces),
        out_shape=(whole, whole),
        in_specs=[hold, hold, leave],
        out_specs=[leave, leave],
        scratch_shapes=[
            pltpu.VMEM(back.shape, jnp.float32),
            pltpu.SemaphoreType.DMA((pieces,)), pltpu.SemaphoreType.DMA((pieces,)),
        ],
        compiler_params=pltpu.CompilerParams(vmem_limit_bytes=FINISH_LIMIT),
        cost_estimate=pl.CostEstimate(flops=2 * back.size, bytes_accessed=20 * back.size, transcendentals=0),
    )(back, weights, new_momentum)


def on_device(n, k, gradients, momentum, weights):
    back, new_momentum = by_kernel(n, k, gradients, momentum)
    return tuple(finish(n, back, weights, new_momentum))


def solution(mesh):
    placed = P(None, "shard", "model")
    return jax.shard_map(
        functools.partial(on_device, mesh.shape["shard"], mesh.shape["model"]),
        mesh=mesh,
        in_specs=(placed, placed, placed),
        out_specs=(placed, placed),
        check_vma=False,
    )
```

```python
import functools

import jax
import jax.numpy as jnp
from jax import lax
from jax.experimental import pallas as pl
from jax.experimental.pallas import tpu as pltpu
from jax.sharding import PartitionSpec as P

ITERS = 4
VMEM_LIMIT = 40 * 1024 * 1024
FINISH_LIMIT = 16 * 1024 * 1024
MESH = pl.DeviceIdType.MESH
HIGHEST = lax.Precision.HIGHEST


hold_rate = 0.8
learn_rate = 1.0


def mm(a, b):
    return jnp.dot(a, b, precision=HIGHEST, preferred_element_type=jnp.float32)


def direction(gram):
    side = gram.shape[-1]
    row = lax.broadcasted_iota(jnp.int32, (side, side), 0)
    col = lax.broadcasted_iota(jnp.int32, (side, side), 1)
    diagonal = row == col
    squares = jnp.sum(jnp.where(diagonal, gram, 0.0), axis=(0, 1), keepdims=True)
    scale = lax.rsqrt(squares + 1e-06)
    a = gram * scale * scale
    q = jnp.where(diagonal, jnp.broadcast_to(scale, gram.shape), 0.0)
    for step in range(ITERS):
        mixed = -4.775 * a + 2.0315 * mm(a, a)
        if step == 0:
            q_next = 3.4445 * q + mixed * scale
        else:
            q_next = 3.4445 * q + mm(mixed, q)
        if step < ITERS - 1:
            half = 3.4445 * a + mm(mixed, a)
            a = 3.4445 * half + mm(mixed, half)
        q = q_next
    return q


def partner(me, off, n):
    if n & (n - 1):
        return lax.rem(me + off, n)
    for bit in range(n.bit_length() - 1):
        if (off >> bit) & 1:
            me = me + (1 - 2 * ((me // (1 << bit)) % 2)) * (1 << bit)
    return me


def partners(me, n):
    offs = range(n - 1, 0, -1)
    if n & (n - 1) or n < 8:
        return [(off, partner(me, off, n)) for off in offs]
    high, next_high = me // (n // 2), me // (n // 4) % 2
    inner = lax.rem(high + next_high, 2)
    found = []
    for off in offs:
        if off < n // 2:
            found.append((off, partner(me, off, n)))
        else:
            other = off ^ (n // 4)
            found.append((off + inner * (other - off),
                          partner(me, off, n) + inner * (partner(me, other, n) - partner(me, off, n))))
    return found


def exchange_kernel(n, k, g_ref, m_ref, w_ref, done_ref, new_ref, grad, held, weight, result, grams,
                    l_grad, l_moved, l_weight, f_send, f_recv, g_send, g_recv, b_send, b_recv, met, go):
    me = lax.axis_index("shard")
    col = lax.axis_index("model")
    local, _, rows, wide = held.shape
    side = n * rows
    early = n >= 8 and n & (n - 1) == 0
    middle = jnp.logical_and(me >= n // 2 - 2, me <= n // 2 + 1)
    hub = me == 0
    facing = (n - 1, n - 2)

    def chunk(j):
        return pl.ds(j * n, n)

    def load_grad(j):
        return pltpu.make_async_copy(g_ref.at[chunk(j)], grad.at[j], l_grad.at[j])

    def load_moved(j):
        return pltpu.make_async_copy(m_ref.at[chunk(j)], new_ref.at[chunk(j)], l_moved.at[j])

    def load_weight():
        return pltpu.make_async_copy(w_ref, weight, l_weight)

    def forward(j, off, to):
        return pltpu.make_async_remote_copy(
            src_ref=new_ref.at[j * n + to], dst_ref=held.at[j, me],
            send_sem=f_send, recv_sem=f_recv.at[j],
            device_id={"shard": to}, device_id_type=MESH)

    def share(j, off):
        return pltpu.make_async_remote_copy(
            src_ref=grams.at[j, col], dst_ref=grams.at[j, col],
            send_sem=g_send, recv_sem=g_recv.at[j],
            device_id={"model": partner(col, off, k)}, device_id_type=MESH)

    def backward(j, off, to):
        return pltpu.make_async_remote_copy(
            src_ref=result.at[j, to], dst_ref=done_ref.at[j * n + me],
            send_sem=b_send, recv_sem=b_recv.at[j],
            device_id={"shard": to}, device_id_type=MESH)

    def drain(ref, semaphore):
        pltpu.make_async_copy(ref, ref, semaphore).wait()

    def signal(semaphore, **to):
        pl.semaphore_signal(semaphore, inc=1, device_id=to, device_id_type=MESH)

    barrier = pltpu.get_barrier_semaphore()
    if early:
        @pl.when(middle)
        def _():
            for off in facing:
                signal(barrier, shard=partner(me, off, n))

        @pl.when(jnp.logical_not(hub))
        def _():
            signal(barrier, shard=0)

        @pl.when(hub)
        def _():
            for off in range(1, k):
                signal(barrier, model=partner(col, off, k))
            for to in range(1, n):
                if not n // 2 - 2 <= to <= n // 2 + 1:
                    signal(barrier, shard=to)
    else:
        for off in range(n - 1, 0, -1):
            signal(barrier, shard=partner(me, off, n))
        for off in range(1, k):
            signal(barrier, model=partner(col, off, k))

    @pl.loop(0, local)
    def _(j):
        load_moved(j).start()
        load_grad(j).start()

    def step(j):
        load_moved(j).wait()
        load_grad(j).wait()
        new_ref[chunk(j)] = hold_rate * new_ref[chunk(j)] + grad[j]

    def send_facing(j):
        @pl.when(middle)
        def _():
            for off in facing:
                forward(j, off, partner(me, off, n)).start()

    def send(j):
        for off, to in partners(me, n):
            if early:
                @pl.when(jnp.logical_not(jnp.logical_and(middle, off >= n - 2)))
                def _():
                    forward(j, off, to).start()
            else:
                forward(j, off, to).start()

    step(0)
    if early:
        pl.semaphore_wait(barrier, jnp.where(hub, n + k - 2, jnp.where(middle, 2, 1)))
        send_facing(0)
    else:
        pl.semaphore_wait(barrier, n + k - 2)

    @pl.loop(1, local)
    def _(j):
        step(j)
        if early:
            send_facing(j)

    if early:
        @pl.when(hub)
        def _():
            for off in range(1, k):
                signal(met, model=partner(col, off, k))
            pl.semaphore_wait(met, k - 1)
            for to in range(n - 1, 0, -1):
                signal(go, shard=to)

        @pl.when(jnp.logical_not(hub))
        def _():
            pl.semaphore_wait(go, 1)

    @pl.loop(0, local)
    def _(j):
        send(j)

    load_weight().start()

    @pl.loop(0, local)
    def _(j):
        held[j, me] = new_ref[j * n + me]
        drain(held.at[j, pl.ds(0, n - 1)], f_recv.at[j])
        x = held[j].reshape(side, wide)
        grams[j, col] = lax.dot_general(
            x, x, (((1,), (1,)), ((), ())), precision=HIGHEST, preferred_element_type=jnp.float32)
        for off in range(1, k):
            share(j, off).start()
        drain(grams.at[j, pl.ds(0, k - 1)], g_recv.at[j])
        gram = grams[j, 0]
        for i in range(1, k):
            gram = gram + grams[j, i]
        result[j] = mm(direction(gram), x).reshape(n, rows, wide)
        for off, to in partners(me, n):
            backward(j, off, to).start()
        done_ref[j * n + me] = result[j, me]

    load_weight().wait()

    @pl.loop(0, local)
    def _(j):
        drain(done_ref.at[pl.ds(j * n, n - 1)], b_recv.at[j])
        done_ref[chunk(j)] = weight[chunk(j)] - learn_rate * done_ref[chunk(j)]

    drain(new_ref.at[pl.ds(0, local * (n - 1))], f_send)
    drain(grams.at[:, pl.ds(0, k - 1)], g_send)
    drain(new_ref.at[pl.ds(0, local * (n - 1))], b_send)


def by_kernel(n, k, gradients, momentum, weights):
    mats, rows, wide = gradients.shape
    local = mats // n
    side = n * rows
    dma = pltpu.SemaphoreType.DMA
    whole = jax.ShapeDtypeStruct(gradients.shape, jnp.float32)
    return pl.pallas_call(
        functools.partial(exchange_kernel, n, k),
        out_shape=(whole, whole),
        in_specs=[pl.BlockSpec(memory_space=pltpu.HBM)] * 3,
        out_specs=[pl.BlockSpec(memory_space=pltpu.VMEM)] * 2,
        scratch_shapes=[
            *[pltpu.VMEM((local, n, rows, wide), jnp.float32)] * 2,
            pltpu.VMEM(gradients.shape, jnp.float32),
            pltpu.VMEM((local, n, rows, wide), jnp.float32),
            pltpu.VMEM((local, k, side, side), jnp.float32),
            dma((local,)), dma((local,)), dma(()),
            dma(()), dma((local,)),
            dma(()), dma((local,)),
            dma(()), dma((local,)),
            pltpu.SemaphoreType.REGULAR, pltpu.SemaphoreType.REGULAR,
        ],
        compiler_params=pltpu.CompilerParams(
            collective_id=0, has_side_effects=True, vmem_limit_bytes=VMEM_LIMIT),
    )(*[pltpu.with_memory_space_constraint(a, pltpu.HBM) for a in (gradients, momentum, weights)])


def finish_kernel(pieces, done_ref, new_ref, out_w, out_new, semaphores):
    step = done_ref.shape[0] // pieces
    copies = []
    for i in range(pieces):
        part = pl.ds(i * step, step)
        for source, target in ((done_ref, out_w), (new_ref, out_new)):
            copies.append(pltpu.make_async_copy(source.at[part], target.at[part], semaphores.at[len(copies)]))
    for copy in copies:
        copy.start()
    for copy in copies:
        copy.wait()


def finish(pieces, done, new_momentum):
    whole = jax.ShapeDtypeStruct(done.shape, jnp.float32)
    return pl.pallas_call(
        functools.partial(finish_kernel, pieces),
        out_shape=(whole, whole),
        in_specs=[pl.BlockSpec(memory_space=pltpu.VMEM)] * 2,
        out_specs=[pl.BlockSpec(memory_space=pl.ANY)] * 2,
        scratch_shapes=[pltpu.SemaphoreType.DMA((2 * pieces,))],
        compiler_params=pltpu.CompilerParams(vmem_limit_bytes=FINISH_LIMIT),
        cost_estimate=pl.CostEstimate(flops=2 * done.size, bytes_accessed=16 * done.size, transcendentals=0),
    )(done, new_momentum)


def on_device(n, k, gradients, momentum, weights):
    done, new_momentum = by_kernel(n, k, gradients, momentum, weights)
    return tuple(finish(2, done, new_momentum))


def solution(mesh):
    placed = P(None, "shard", "model")
    return jax.shard_map(
        functools.partial(on_device, mesh.shape["shard"], mesh.shape["model"]),
        mesh=mesh,
        in_specs=(placed, placed, placed),
        out_specs=(placed, placed),
        check_vma=False,
    )
```

```python
import functools

import jax
import jax.numpy as jnp
from jax import lax
from jax.experimental import pallas as pl
from jax.experimental.pallas import tpu as pltpu
from jax.sharding import PartitionSpec as P

ITERS = 4
VMEM_LIMIT = 40 * 1024 * 1024
FINISH_LIMIT = 16 * 1024 * 1024
MESH = pl.DeviceIdType.MESH
HIGHEST = lax.Precision.HIGHEST


hold_rate = 0.8
learn_rate = 1.0


def mm(a, b):
    return jnp.dot(a, b, precision=HIGHEST, preferred_element_type=jnp.float32)


def direction(gram):
    side = gram.shape[-1]
    row = lax.broadcasted_iota(jnp.int32, (side, side), 0)
    col = lax.broadcasted_iota(jnp.int32, (side, side), 1)
    diagonal = row == col
    squares = jnp.sum(jnp.where(diagonal, gram, 0.0), axis=(0, 1), keepdims=True)
    scale = lax.rsqrt(squares + 1e-06)
    a = gram * scale * scale
    q = jnp.where(diagonal, jnp.broadcast_to(scale, gram.shape), 0.0)
    for step in range(ITERS):
        mixed = -4.775 * a + 2.0315 * mm(a, a)
        if step == 0:
            q_next = 3.4445 * q + mixed * scale
        else:
            q_next = 3.4445 * q + mm(mixed, q)
        if step < ITERS - 1:
            half = 3.4445 * a + mm(mixed, a)
            a = 3.4445 * half + mm(mixed, half)
        q = q_next
    return q


def partner(me, off, n):
    if n & (n - 1):
        return lax.rem(me + off, n)
    for bit in range(n.bit_length() - 1):
        if (off >> bit) & 1:
            me = me + (1 - 2 * ((me // (1 << bit)) % 2)) * (1 << bit)
    return me


def partners(me, n):
    offs = range(n - 1, 0, -1)
    if n & (n - 1) or n < 8:
        return [(off, partner(me, off, n)) for off in offs]
    high, next_high = me // (n // 2), me // (n // 4) % 2
    inner = lax.rem(high + next_high, 2)
    found = []
    for off in offs:
        if off < n // 2:
            found.append((off, partner(me, off, n)))
        else:
            other = off ^ (n // 4)
            found.append((off + inner * (other - off),
                          partner(me, off, n) + inner * (partner(me, other, n) - partner(me, off, n))))
    return found


def across(me, n, upper):
    if n & (n - 1) or n < 8:
        return []
    quarter = n // 4
    shift = lax.rem(me // quarter + upper, 2) * quarter
    start = me // (2 * quarter) * -2 * quarter + (2 * quarter)
    return [(off + shift, start + upper * quarter + inner_place(me, off, quarter))
            for off in range(3 * quarter - 1, 2 * quarter - 1, -1)]


def inner_place(me, off, quarter):
    return partner(lax.rem(me, quarter), off % quarter, quarter)


def within(me, n):
    top = n - 1 if n & (n - 1) or n < 8 else n // 2 - 1
    return [(off, partner(me, off, n)) for off in range(top, 0, -1)]


def exchange_kernel(n, k, g_ref, m_ref, w_ref, done_ref, new_ref, grad, held, weight, result, grams, first,
                    l_grad, l_moved, l_weight, l_first, f_send, f_recv, g_send, g_recv, b_send, b_recv, near, met, go):
    me = lax.axis_index("shard")
    col = lax.axis_index("model")
    local, _, rows, wide = held.shape
    side = n * rows
    early = n >= 8 and n & (n - 1) == 0
    middle = jnp.logical_and(me >= n // 2 - 2, me <= n // 2 + 1)
    hub = me == 0
    across_off, opposite_off = n - 1, n - 2
    opposite = partner(me, opposite_off, n)

    def chunk(j):
        return pl.ds(j * n, n)

    def load_grad(j):
        return pltpu.make_async_copy(g_ref.at[chunk(j)], grad.at[j], l_grad.at[j])

    def load_moved(j):
        return pltpu.make_async_copy(m_ref.at[chunk(j)], new_ref.at[chunk(j)], l_moved.at[j])

    def load_first(i, ref):
        return pltpu.make_async_copy(ref.at[opposite], first.at[i], l_first.at[i])

    def load_weight():
        return pltpu.make_async_copy(w_ref, weight, l_weight)

    def forward(j, off, to, source=None):
        return pltpu.make_async_remote_copy(
            src_ref=new_ref.at[j * n + to] if source is None else source, dst_ref=held.at[j, me],
            send_sem=f_send, recv_sem=f_recv.at[j],
            device_id={"shard": to}, device_id_type=MESH)

    def share(j, off):
        return pltpu.make_async_remote_copy(
            src_ref=grams.at[j, col], dst_ref=grams.at[j, col],
            send_sem=g_send, recv_sem=g_recv.at[j],
            device_id={"model": partner(col, off, k)}, device_id_type=MESH)

    def backward(j, off, to):
        return pltpu.make_async_remote_copy(
            src_ref=result.at[j, to], dst_ref=done_ref.at[j * n + me],
            send_sem=b_send, recv_sem=b_recv.at[j],
            device_id={"shard": to}, device_id_type=MESH)

    def drain(ref, semaphore):
        pltpu.make_async_copy(ref, ref, semaphore).wait()

    def signal(semaphore, **to):
        pl.semaphore_signal(semaphore, inc=1, device_id=to, device_id_type=MESH)

    barrier = pltpu.get_barrier_semaphore()
    if early:
        @pl.when(middle)
        def _():
            signal(barrier, shard=opposite)
            signal(barrier, shard=partner(me, 1, n))

        @pl.when(jnp.logical_not(hub))
        def _():
            signal(barrier, shard=0)

        @pl.when(hub)
        def _():
            for off in range(1, k):
                signal(barrier, model=partner(col, off, k))
            for to in range(1, n):
                if not n // 2 - 2 <= to <= n // 2 + 1:
                    signal(barrier, shard=to)
    else:
        for off in range(n - 1, 0, -1):
            signal(barrier, shard=partner(me, off, n))
        for off in range(1, k):
            signal(barrier, model=partner(col, off, k))

    if early:
        load_first(0, m_ref).start()
        load_first(1, g_ref).start()

    @pl.loop(0, local)
    def _(j):
        load_moved(j).start()
        load_grad(j).start()

    def step(j):
        load_moved(j).wait()
        load_grad(j).wait()
        new_ref[chunk(j)] = hold_rate * new_ref[chunk(j)] + grad[j]

    def send(j):
        for off, to in partners(me, n):
            if early:
                @pl.when(jnp.logical_not(jnp.logical_and(middle, off >= n - 2)))
                def _():
                    forward(j, off, to).start()
            else:
                forward(j, off, to).start()

    if early:
        load_first(0, m_ref).wait()
        load_first(1, g_ref).wait()
        first[0] = hold_rate * first[0] + first[1]
        pl.semaphore_wait(barrier, jnp.where(hub, n + k - 2, jnp.where(middle, 2, 1)))

        @pl.when(middle)
        def _():
            forward(0, opposite_off, opposite, first.at[0]).start()
            signal(near, shard=partner(me, 1, n))

        @pl.loop(1, local)
        def _(j):
            step(j)

            @pl.when(middle)
            def _():
                forward(j, opposite_off, opposite).start()

        step(0)

        @pl.when(middle)
        def _():
            pl.semaphore_wait(near, 1)

            @pl.loop(0, local)
            def _(j):
                forward(j, across_off, partner(me, across_off, n)).start()
    else:
        step(0)
        pl.semaphore_wait(barrier, n + k - 2)

        @pl.loop(1, local)
        def _(j):
            step(j)

    if early:
        @pl.when(hub)
        def _():
            for off in range(1, k):
                signal(met, model=partner(col, off, k))
            pl.semaphore_wait(met, k - 1)
            for to in range(n - 1, 0, -1):
                signal(go, shard=to)

        @pl.when(jnp.logical_not(hub))
        def _():
            pl.semaphore_wait(go, 1)

    @pl.loop(0, local)
    def _(j):
        send(j)

    load_weight().start()

    @pl.loop(0, local)
    def _(j):
        held[j, me] = new_ref[j * n + me]
        drain(held.at[j, pl.ds(0, n - 1)], f_recv.at[j])
        x = held[j].reshape(side, wide)
        grams[j, col] = lax.dot_general(
            x, x, (((1,), (1,)), ((), ())), precision=HIGHEST, preferred_element_type=jnp.float32)
        for off in range(1, k):
            share(j, off).start()
        drain(grams.at[j, pl.ds(0, k - 1)], g_recv.at[j])
        gram = grams[j, 0]
        for i in range(1, k):
            gram = gram + grams[j, i]
        result[j] = mm(direction(gram), x).reshape(n, rows, wide)
        for off, to in across(me, n, 0):
            backward(j, off, to).start()

        @pl.when(jnp.logical_or(j < local - 2, j == local - 1))
        def _():
            @pl.loop(jnp.where(j == local - 1, max(local - 2, 0), j), j + 1)
            def _(i):
                for off, to in across(me, n, 1):
                    backward(i, off, to).start()

        for off, to in within(me, n):
            backward(j, off, to).start()
        done_ref[j * n + me] = result[j, me]

    load_weight().wait()

    @pl.loop(0, local)
    def _(j):
        drain(done_ref.at[pl.ds(j * n, n - 1)], b_recv.at[j])
        done_ref[chunk(j)] = weight[chunk(j)] - learn_rate * done_ref[chunk(j)]

    drain(new_ref.at[pl.ds(0, local * (n - 1))], f_send)
    drain(grams.at[:, pl.ds(0, k - 1)], g_send)
    drain(new_ref.at[pl.ds(0, local * (n - 1))], b_send)


def by_kernel(n, k, gradients, momentum, weights):
    mats, rows, wide = gradients.shape
    local = mats // n
    side = n * rows
    dma = pltpu.SemaphoreType.DMA
    whole = jax.ShapeDtypeStruct(gradients.shape, jnp.float32)
    return pl.pallas_call(
        functools.partial(exchange_kernel, n, k),
        out_shape=(whole, whole),
        in_specs=[pl.BlockSpec(memory_space=pltpu.HBM)] * 3,
        out_specs=[pl.BlockSpec(memory_space=pltpu.VMEM)] * 2,
        scratch_shapes=[
            *[pltpu.VMEM((local, n, rows, wide), jnp.float32)] * 2,
            pltpu.VMEM(gradients.shape, jnp.float32),
            pltpu.VMEM((local, n, rows, wide), jnp.float32),
            pltpu.VMEM((local, k, side, side), jnp.float32),
            pltpu.VMEM((2, rows, wide), jnp.float32),
            dma((local,)), dma((local,)), dma(()), dma((2,)),
            dma(()), dma((local,)),
            dma(()), dma((local,)),
            dma(()), dma((local,)),
            *[pltpu.SemaphoreType.REGULAR] * 3,
        ],
        compiler_params=pltpu.CompilerParams(
            collective_id=0, has_side_effects=True, vmem_limit_bytes=VMEM_LIMIT),
    )(*[pltpu.with_memory_space_constraint(a, pltpu.HBM) for a in (gradients, momentum, weights)])


def finish_kernel(pieces, done_ref, new_ref, out_w, out_new, semaphores):
    step = done_ref.shape[0] // pieces
    copies = []
    for i in range(pieces):
        part = pl.ds(i * step, step)
        for source, target in ((done_ref, out_w), (new_ref, out_new)):
            copies.append(pltpu.make_async_copy(source.at[part], target.at[part], semaphores.at[len(copies)]))
    for copy in copies:
        copy.start()
    for copy in copies:
        copy.wait()


def finish(pieces, done, new_momentum):
    whole = jax.ShapeDtypeStruct(done.shape, jnp.float32)
    return pl.pallas_call(
        functools.partial(finish_kernel, pieces),
        out_shape=(whole, whole),
        in_specs=[pl.BlockSpec(memory_space=pltpu.VMEM)] * 2,
        out_specs=[pl.BlockSpec(memory_space=pl.ANY)] * 2,
        scratch_shapes=[pltpu.SemaphoreType.DMA((2 * pieces,))],
        compiler_params=pltpu.CompilerParams(vmem_limit_bytes=FINISH_LIMIT),
        cost_estimate=pl.CostEstimate(flops=2 * done.size, bytes_accessed=16 * done.size, transcendentals=0),
    )(done, new_momentum)


def on_device(n, k, gradients, momentum, weights):
    done, new_momentum = by_kernel(n, k, gradients, momentum, weights)
    return tuple(finish(2, done, new_momentum))


def solution(mesh):
    placed = P(None, "shard", "model")
    return jax.shard_map(
        functools.partial(on_device, mesh.shape["shard"], mesh.shape["model"]),
        mesh=mesh,
        in_specs=(placed, placed, placed),
        out_specs=(placed, placed),
        check_vma=False,
    )
```

```python
import functools

import jax
import jax.numpy as jnp
from jax import lax
from jax.experimental import pallas as pl
from jax.experimental.pallas import tpu as pltpu
from jax.sharding import PartitionSpec as P

ITERS = 4
VMEM_LIMIT = 40 * 1024 * 1024
FINISH_LIMIT = 16 * 1024 * 1024
MESH = pl.DeviceIdType.MESH
HIGHEST = lax.Precision.HIGHEST


hold_rate = 0.8
learn_rate = 1.0


def mm(a, b):
    return jnp.dot(a, b, precision=HIGHEST, preferred_element_type=jnp.float32)


def direction(gram):
    side = gram.shape[-1]
    row = lax.broadcasted_iota(jnp.int32, (side, side), 0)
    col = lax.broadcasted_iota(jnp.int32, (side, side), 1)
    diagonal = row == col
    squares = jnp.sum(jnp.where(diagonal, gram, 0.0), axis=(0, 1), keepdims=True)
    scale = lax.rsqrt(squares + 1e-06)
    a = gram * scale * scale
    q = jnp.where(diagonal, jnp.broadcast_to(scale, gram.shape), 0.0)
    for step in range(ITERS):
        mixed = -4.775 * a + 2.0315 * mm(a, a)
        if step == 0:
            q_next = 3.4445 * q + mixed * scale
        else:
            q_next = 3.4445 * q + mm(mixed, q)
        if step < ITERS - 1:
            half = 3.4445 * a + mm(mixed, a)
            a = 3.4445 * half + mm(mixed, half)
        q = q_next
    return q


def partner(me, off, n):
    if n & (n - 1):
        return lax.rem(me + off, n)
    for bit in range(n.bit_length() - 1):
        if (off >> bit) & 1:
            me = me + (1 - 2 * ((me // (1 << bit)) % 2)) * (1 << bit)
    return me


def partners(me, n):
    offs = range(n - 1, 0, -1)
    if n & (n - 1) or n < 8:
        return [(off, partner(me, off, n)) for off in offs]
    high, next_high = me // (n // 2), me // (n // 4) % 2
    inner = lax.rem(high + next_high, 2)
    found = []
    for off in offs:
        if off < n // 2:
            found.append((off, partner(me, off, n)))
        else:
            other = off ^ (n // 4)
            found.append((off + inner * (other - off),
                          partner(me, off, n) + inner * (partner(me, other, n) - partner(me, off, n))))
    return found


def across(me, n, upper):
    if n & (n - 1) or n < 8:
        return []
    quarter = n // 4
    shift = lax.rem(me // quarter + upper, 2) * quarter
    start = me // (2 * quarter) * -2 * quarter + (2 * quarter)
    return [(off + shift, start + upper * quarter + inner_place(me, off, quarter))
            for off in range(3 * quarter - 1, 2 * quarter - 1, -1)]


def inner_place(me, off, quarter):
    return partner(lax.rem(me, quarter), off % quarter, quarter)


def within(me, n):
    top = n - 1 if n & (n - 1) or n < 8 else n // 2 - 1
    return [(off, partner(me, off, n)) for off in range(top, 0, -1)]


def exchange_kernel(n, k, g_ref, m_ref, w_ref, done_ref, new_ref, grad, held, weight, result, grams, first,
                    l_grad, l_moved, l_weight, l_first, f_send, f_recv, g_send, g_recv, b_send, b_recv, near, met, go):
    me = lax.axis_index("shard")
    col = lax.axis_index("model")
    local, _, rows, wide = held.shape
    side = n * rows
    early = n >= 8 and n & (n - 1) == 0
    middle = jnp.logical_and(me >= n // 2 - 2, me <= n // 2 + 1)
    lower = jnp.logical_and(middle, me < n // 2)
    hub = me == 0
    across_off, opposite_off = n - 1, n - 2
    opposite = partner(me, opposite_off, n)
    late = lax.rem(col, 2) == 1
    prompt = jnp.logical_and(middle, jnp.logical_not(late))

    def chunk(j):
        return pl.ds(j * n, n)

    def load_grad(j):
        return pltpu.make_async_copy(g_ref.at[chunk(j)], grad.at[j], l_grad.at[j])

    def load_moved(j):
        return pltpu.make_async_copy(m_ref.at[chunk(j)], new_ref.at[chunk(j)], l_moved.at[j])

    def load_first(i, ref):
        return pltpu.make_async_copy(ref.at[opposite], first.at[i], l_first.at[i])

    def load_weight():
        return pltpu.make_async_copy(w_ref, weight, l_weight)

    def forward(j, off, to, source=None):
        return pltpu.make_async_remote_copy(
            src_ref=new_ref.at[j * n + to] if source is None else source, dst_ref=held.at[j, me],
            send_sem=f_send, recv_sem=f_recv.at[j],
            device_id={"shard": to}, device_id_type=MESH)

    def share(j, off):
        return pltpu.make_async_remote_copy(
            src_ref=grams.at[j, col], dst_ref=grams.at[j, col],
            send_sem=g_send, recv_sem=g_recv.at[j],
            device_id={"model": partner(col, off, k)}, device_id_type=MESH)

    def backward(j, off, to):
        return pltpu.make_async_remote_copy(
            src_ref=result.at[j, to], dst_ref=done_ref.at[j * n + me],
            send_sem=b_send, recv_sem=b_recv.at[j],
            device_id={"shard": to}, device_id_type=MESH)

    def drain(ref, semaphore):
        pltpu.make_async_copy(ref, ref, semaphore).wait()

    def signal(semaphore, **to):
        pl.semaphore_signal(semaphore, inc=1, device_id=to, device_id_type=MESH)

    barrier = pltpu.get_barrier_semaphore()
    if early:
        load_first(0, m_ref).start()
        load_first(1, g_ref).start()

        @pl.when(middle)
        def _():
            signal(barrier, shard=opposite)

        @pl.when(lower)
        def _():
            signal(barrier, shard=partner(me, 1, n))

        @pl.when(jnp.logical_not(hub))
        def _():
            signal(barrier, shard=0)

        @pl.when(hub)
        def _():
            for off in range(1, k):
                signal(barrier, model=partner(col, off, k))
            for to in range(1, n):
                if not n // 2 - 2 <= to <= n // 2 + 1:
                    signal(barrier, shard=to)
    else:
        for off in range(n - 1, 0, -1):
            signal(barrier, shard=partner(me, off, n))
        for off in range(1, k):
            signal(barrier, model=partner(col, off, k))

    @pl.loop(0, local)
    def _(j):
        load_moved(j).start()
        load_grad(j).start()

    def step(j):
        load_moved(j).wait()
        load_grad(j).wait()
        new_ref[chunk(j)] = hold_rate * new_ref[chunk(j)] + grad[j]

    def send(j):
        for off, to in partners(me, n):
            if early:
                @pl.when(jnp.logical_not(jnp.logical_and(middle, off >= n - 2)))
                def _():
                    forward(j, off, to).start()
            else:
                forward(j, off, to).start()

    if early:
        load_first(0, m_ref).wait()
        load_first(1, g_ref).wait()
        first[0] = hold_rate * first[0] + first[1]
        pl.semaphore_wait(barrier, jnp.where(hub, n + k - 2, jnp.where(lower, 2, 1)))

        @pl.when(middle)
        def _():
            forward(0, opposite_off, opposite, first.at[0]).start()

        @pl.when(lower)
        def _():
            signal(near, shard=partner(me, 1, n))
            signal(near, shard=opposite)

        @pl.loop(1, local)
        def _(j):
            step(j)

            @pl.when(jnp.logical_and(middle, jnp.logical_or(jnp.logical_not(late), j < local - 1)))
            def _():
                forward(j, opposite_off, opposite).start()

        step(0)

        @pl.when(middle)
        def _():
            pl.semaphore_wait(near, 1)

        @pl.when(prompt)
        def _():
            @pl.loop(0, local)
            def _(j):
                forward(j, across_off, partner(me, across_off, n)).start()
    else:
        step(0)
        pl.semaphore_wait(barrier, n + k - 2)

        @pl.loop(1, local)
        def _(j):
            step(j)

    if early:
        @pl.when(hub)
        def _():
            for off in range(1, k):
                signal(met, model=partner(col, off, k))
            pl.semaphore_wait(met, k - 1)
            for to in range(n - 1, 0, -1):
                signal(go, shard=to)

        @pl.when(jnp.logical_not(hub))
        def _():
            pl.semaphore_wait(go, 1)

    if early:
        @pl.when(jnp.logical_and(middle, late))
        def _():
            @pl.loop(max(local - 1, 1), local)
            def _(j):
                forward(j, opposite_off, opposite).start()

            @pl.loop(0, local)
            def _(j):
                forward(j, across_off, partner(me, across_off, n)).start()

    @pl.loop(0, local)
    def _(j):
        send(j)

    load_weight().start()

    @pl.loop(0, local)
    def _(j):
        held[j, me] = new_ref[j * n + me]
        drain(held.at[j, pl.ds(0, n - 1)], f_recv.at[j])
        x = held[j].reshape(side, wide)
        grams[j, col] = lax.dot_general(
            x, x, (((1,), (1,)), ((), ())), precision=HIGHEST, preferred_element_type=jnp.float32)
        for off in range(1, k):
            share(j, off).start()
        drain(grams.at[j, pl.ds(0, k - 1)], g_recv.at[j])
        gram = grams[j, 0]
        for i in range(1, k):
            gram = gram + grams[j, i]
        result[j] = mm(direction(gram), x).reshape(n, rows, wide)
        for off, to in across(me, n, 0):
            backward(j, off, to).start()

        @pl.when(jnp.logical_or(j < local - 2, j == local - 1))
        def _():
            @pl.loop(jnp.where(j == local - 1, max(local - 2, 0), j), j + 1)
            def _(i):
                for off, to in across(me, n, 1):
                    backward(i, off, to).start()

        for off, to in within(me, n):
            backward(j, off, to).start()
        done_ref[j * n + me] = result[j, me]

    load_weight().wait()

    @pl.loop(0, local)
    def _(j):
        drain(done_ref.at[pl.ds(j * n, n - 1)], b_recv.at[j])
        done_ref[chunk(j)] = weight[chunk(j)] - learn_rate * done_ref[chunk(j)]

    drain(new_ref.at[pl.ds(0, local * (n - 1))], f_send)
    drain(grams.at[:, pl.ds(0, k - 1)], g_send)
    drain(new_ref.at[pl.ds(0, local * (n - 1))], b_send)


def by_kernel(n, k, gradients, momentum, weights):
    mats, rows, wide = gradients.shape
    local = mats // n
    side = n * rows
    dma = pltpu.SemaphoreType.DMA
    whole = jax.ShapeDtypeStruct(gradients.shape, jnp.float32)
    return pl.pallas_call(
        functools.partial(exchange_kernel, n, k),
        out_shape=(whole, whole),
        in_specs=[pl.BlockSpec(memory_space=pltpu.HBM)] * 3,
        out_specs=[pl.BlockSpec(memory_space=pltpu.VMEM)] * 2,
        scratch_shapes=[
            *[pltpu.VMEM((local, n, rows, wide), jnp.float32)] * 2,
            pltpu.VMEM(gradients.shape, jnp.float32),
            pltpu.VMEM((local, n, rows, wide), jnp.float32),
            pltpu.VMEM((local, k, side, side), jnp.float32),
            pltpu.VMEM((2, rows, wide), jnp.float32),
            dma((local,)), dma((local,)), dma(()), dma((2,)),
            dma(()), dma((local,)),
            dma(()), dma((local,)),
            dma(()), dma((local,)),
            *[pltpu.SemaphoreType.REGULAR] * 3,
        ],
        compiler_params=pltpu.CompilerParams(
            collective_id=0, has_side_effects=True, vmem_limit_bytes=VMEM_LIMIT),
    )(*[pltpu.with_memory_space_constraint(a, pltpu.HBM) for a in (gradients, momentum, weights)])


def finish_kernel(pieces, done_ref, new_ref, out_w, out_new, semaphores):
    step = done_ref.shape[0] // pieces
    copies = []
    for i in range(pieces):
        part = pl.ds(i * step, step)
        for source, target in ((done_ref, out_w), (new_ref, out_new)):
            copies.append(pltpu.make_async_copy(source.at[part], target.at[part], semaphores.at[len(copies)]))
    for copy in copies:
        copy.start()
    for copy in copies:
        copy.wait()


def finish(pieces, done, new_momentum):
    whole = jax.ShapeDtypeStruct(done.shape, jnp.float32)
    return pl.pallas_call(
        functools.partial(finish_kernel, pieces),
        out_shape=(whole, whole),
        in_specs=[pl.BlockSpec(memory_space=pltpu.VMEM)] * 2,
        out_specs=[pl.BlockSpec(memory_space=pl.ANY)] * 2,
        scratch_shapes=[pltpu.SemaphoreType.DMA((2 * pieces,))],
        compiler_params=pltpu.CompilerParams(vmem_limit_bytes=FINISH_LIMIT),
        cost_estimate=pl.CostEstimate(flops=2 * done.size, bytes_accessed=16 * done.size, transcendentals=0),
    )(done, new_momentum)


def on_device(n, k, gradients, momentum, weights):
    done, new_momentum = by_kernel(n, k, gradients, momentum, weights)
    return tuple(finish(2, done, new_momentum))


def solution(mesh):
    placed = P(None, "shard", "model")
    return jax.shard_map(
        functools.partial(on_device, mesh.shape["shard"], mesh.shape["model"]),
        mesh=mesh,
        in_specs=(placed, placed, placed),
        out_specs=(placed, placed),
        check_vma=False,
    )
```

```python
import functools

import jax
import jax.numpy as jnp
from jax import lax
from jax.experimental import pallas as pl
from jax.experimental.pallas import tpu as pltpu
from jax.sharding import PartitionSpec as P

ITERS = 4
VMEM_LIMIT = 40 * 1024 * 1024
FINISH_LIMIT = 16 * 1024 * 1024
MESH = pl.DeviceIdType.MESH
HIGHEST = lax.Precision.HIGHEST


hold_rate = 0.8
learn_rate = 1.0


def mm(a, b):
    return jnp.dot(a, b, precision=HIGHEST, preferred_element_type=jnp.float32)


def direction(gram):
    side = gram.shape[-1]
    row = lax.broadcasted_iota(jnp.int32, (side, side), 0)
    col = lax.broadcasted_iota(jnp.int32, (side, side), 1)
    diagonal = row == col
    squares = jnp.sum(jnp.where(diagonal, gram, 0.0), axis=(0, 1), keepdims=True)
    scale = lax.rsqrt(squares + 1e-06)
    a = gram * scale * scale
    q = jnp.where(diagonal, jnp.broadcast_to(scale, gram.shape), 0.0)
    for step in range(ITERS):
        mixed = -4.775 * a + 2.0315 * mm(a, a)
        if step == 0:
            q_next = 3.4445 * q + mixed * scale
        else:
            q_next = 3.4445 * q + mm(mixed, q)
        if step < ITERS - 1:
            half = 3.4445 * a + mm(mixed, a)
            a = 3.4445 * half + mm(mixed, half)
        q = q_next
    return q


def partner(me, off, n):
    if n & (n - 1):
        return lax.rem(me + off, n)
    for bit in range(n.bit_length() - 1):
        if (off >> bit) & 1:
            me = me + (1 - 2 * ((me // (1 << bit)) % 2)) * (1 << bit)
    return me


def partners(me, n):
    offs = range(n - 1, 0, -1)
    if n & (n - 1) or n < 8:
        return [(off, partner(me, off, n)) for off in offs]
    high, next_high = me // (n // 2), me // (n // 4) % 2
    inner = lax.rem(high + next_high, 2)
    found = []
    for off in offs:
        if off < n // 2:
            found.append((off, partner(me, off, n)))
        else:
            other = off ^ (n // 4)
            found.append((off + inner * (other - off),
                          partner(me, off, n) + inner * (partner(me, other, n) - partner(me, off, n))))
    return found


def across(me, n, upper):
    if n & (n - 1) or n < 8:
        return []
    quarter = n // 4
    shift = lax.rem(me // quarter + upper, 2) * quarter
    start = me // (2 * quarter) * -2 * quarter + (2 * quarter)
    return [(off + shift, start + upper * quarter + inner_place(me, off, quarter))
            for off in range(3 * quarter - 1, 2 * quarter - 1, -1)]


def inner_place(me, off, quarter):
    return partner(lax.rem(me, quarter), off % quarter, quarter)


def within(me, n):
    top = n - 1 if n & (n - 1) or n < 8 else n // 2 - 1
    return [(off, partner(me, off, n)) for off in range(top, 0, -1)]


def exchange_kernel(n, k, g_ref, m_ref, w_ref, done_ref, new_ref, pair, held, weight, result, grams, first,
                    l_pair, l_weight, l_first, f_send, f_recv, g_send, g_recv, b_send, b_recv, near, go):
    me = lax.axis_index("shard")
    col = lax.axis_index("model")
    local, _, rows, wide = held.shape
    side = n * rows
    early = n >= 8 and n & (n - 1) == 0
    middle = jnp.logical_and(me >= n // 2 - 2, me <= n // 2 + 1)
    lower = jnp.logical_and(middle, me < n // 2)
    hub = me == 0
    across_off, opposite_off = n - 1, n - 2
    opposite = partner(me, opposite_off, n)
    late = lax.rem(col, 2) == 1
    prompt = jnp.logical_and(middle, jnp.logical_not(late))

    def chunk(j):
        return pl.ds(j * n, n)

    def load_grad(j):
        return pltpu.make_async_copy(g_ref.at[chunk(j)], pair.at[j, 1], l_pair.at[j])

    def load_moved(j):
        return pltpu.make_async_copy(m_ref.at[chunk(j)], pair.at[j, 0], l_pair.at[j])

    def load_first(i, ref):
        return pltpu.make_async_copy(ref.at[opposite], first.at[i], l_first)

    def load_weight():
        return pltpu.make_async_copy(w_ref, weight, l_weight)

    def forward(j, off, to, source=None):
        return pltpu.make_async_remote_copy(
            src_ref=new_ref.at[j * n + to] if source is None else source, dst_ref=held.at[j, me],
            send_sem=f_send, recv_sem=f_recv.at[j],
            device_id={"shard": to}, device_id_type=MESH)

    def share(j, off):
        return pltpu.make_async_remote_copy(
            src_ref=grams.at[j, col], dst_ref=grams.at[j, col],
            send_sem=g_send, recv_sem=g_recv.at[lax.rem(j, 2)],
            device_id={"model": partner(col, off, k)}, device_id_type=MESH)

    def backward(j, off, to):
        return pltpu.make_async_remote_copy(
            src_ref=result.at[j, to], dst_ref=done_ref.at[j * n + me],
            send_sem=b_send, recv_sem=b_recv.at[j // max(local - 1, 1)],
            device_id={"shard": to}, device_id_type=MESH)

    def drain(ref, semaphore):
        pltpu.make_async_copy(ref, ref, semaphore).wait()

    def signal(semaphore, **to):
        pl.semaphore_signal(semaphore, inc=1, device_id=to, device_id_type=MESH)

    barrier = pltpu.get_barrier_semaphore()
    if early:
        load_first(0, m_ref).start()
        load_first(1, g_ref).start()

        @pl.when(middle)
        def _():
            signal(barrier, shard=opposite)

        @pl.when(lower)
        def _():
            signal(barrier, shard=partner(me, 1, n))

        @pl.when(jnp.logical_not(hub))
        def _():
            signal(barrier, shard=0)

        @pl.when(hub)
        def _():
            for off in range(1, k):
                signal(barrier, model=partner(col, off, k))
            for to in range(1, n):
                if not n // 2 - 2 <= to <= n // 2 + 1:
                    signal(barrier, shard=to)
    else:
        for off in range(n - 1, 0, -1):
            signal(barrier, shard=partner(me, off, n))
        for off in range(1, k):
            signal(barrier, model=partner(col, off, k))

    @pl.loop(0, local)
    def _(j):
        load_moved(j).start()
        load_grad(j).start()

    def step(j):
        drain(pair.at[j], l_pair.at[j])
        new_ref[chunk(j)] = hold_rate * pair[j, 0] + pair[j, 1]

    def send(j):
        for off, to in partners(me, n):
            if early:
                @pl.when(jnp.logical_not(jnp.logical_and(middle, off >= n - 2)))
                def _():
                    forward(j, off, to).start()
            else:
                forward(j, off, to).start()

    if early:
        drain(first, l_first)
        first[0] = hold_rate * first[0] + first[1]
        pl.semaphore_wait(barrier, jnp.where(hub, n + k - 2, jnp.where(lower, 2, 1)))

        @pl.when(middle)
        def _():
            forward(0, opposite_off, opposite, first.at[0]).start()

        @pl.when(lower)
        def _():
            signal(near, shard=partner(me, 1, n))
            signal(near, shard=opposite)

        @pl.loop(1, local)
        def _(j):
            step(j)

            @pl.when(jnp.logical_and(middle, jnp.logical_or(jnp.logical_not(late), j < local - 1)))
            def _():
                forward(j, opposite_off, opposite).start()

        step(0)

        @pl.when(middle)
        def _():
            pl.semaphore_wait(near, 1)

        @pl.when(prompt)
        def _():
            @pl.loop(0, local)
            def _(j):
                forward(j, across_off, partner(me, across_off, n)).start()
    else:
        step(0)
        pl.semaphore_wait(barrier, n + k - 2)

        @pl.loop(1, local)
        def _(j):
            step(j)

    if early:
        @pl.when(hub)
        def _():
            for off in range(1, k):
                signal(go, model=partner(col, off, k))
            pl.semaphore_wait(go, k - 1)
            for to in range(n - 1, 0, -1):
                signal(go, shard=to)

        @pl.when(jnp.logical_not(hub))
        def _():
            pl.semaphore_wait(go, 1)

    if early:
        @pl.when(jnp.logical_and(middle, late))
        def _():
            @pl.loop(max(local - 1, 1), local)
            def _(j):
                forward(j, opposite_off, opposite).start()

            @pl.loop(0, local)
            def _(j):
                forward(j, across_off, partner(me, across_off, n)).start()

    @pl.loop(0, local)
    def _(j):
        send(j)

    load_weight().start()

    @pl.loop(0, local)
    def _(j):
        held[j, me] = new_ref[j * n + me]
        drain(held.at[j, pl.ds(0, n - 1)], f_recv.at[j])
        x = held[j].reshape(side, wide)
        grams[j, col] = lax.dot_general(
            x, x, (((1,), (1,)), ((), ())), precision=HIGHEST, preferred_element_type=jnp.float32)
        for off in range(1, k):
            share(j, off).start()
        drain(grams.at[j, pl.ds(0, k - 1)], g_recv.at[lax.rem(j, 2)])
        gram = grams[j, 0]
        for i in range(1, k):
            gram = gram + grams[j, i]
        result[j] = mm(direction(gram), x).reshape(n, rows, wide)
        for off, to in across(me, n, 0):
            backward(j, off, to).start()

        @pl.when(jnp.logical_or(j < local - 2, j == local - 1))
        def _():
            @pl.loop(jnp.where(j == local - 1, max(local - 2, 0), j), j + 1)
            def _(i):
                for off, to in across(me, n, 1):
                    backward(i, off, to).start()

        for off, to in within(me, n):
            backward(j, off, to).start()
        done_ref[j * n + me] = result[j, me]

    load_weight().wait()

    def subtract(j):
        done_ref[chunk(j)] = weight[chunk(j)] - learn_rate * done_ref[chunk(j)]

    before = max(local - 1, 1)
    drain(done_ref.at[pl.ds(0, before * (n - 1))], b_recv.at[0])

    @pl.loop(0, before)
    def _(j):
        subtract(j)

    if before < local:
        drain(done_ref.at[pl.ds(0, n - 1)], b_recv.at[1])
        subtract(before)

    drain(new_ref.at[pl.ds(0, local * (n - 1))], f_send)
    drain(grams.at[:, pl.ds(0, k - 1)], g_send)
    drain(new_ref.at[pl.ds(0, local * (n - 1))], b_send)


def by_kernel(n, k, gradients, momentum, weights):
    mats, rows, wide = gradients.shape
    local = mats // n
    side = n * rows
    dma = pltpu.SemaphoreType.DMA
    whole = jax.ShapeDtypeStruct(gradients.shape, jnp.float32)
    return pl.pallas_call(
        functools.partial(exchange_kernel, n, k),
        out_shape=(whole, whole),
        in_specs=[pl.BlockSpec(memory_space=pltpu.HBM)] * 3,
        out_specs=[pl.BlockSpec(memory_space=pltpu.VMEM)] * 2,
        scratch_shapes=[
            pltpu.VMEM((local, 2, n, rows, wide), jnp.float32),
            pltpu.VMEM((local, n, rows, wide), jnp.float32),
            pltpu.VMEM(gradients.shape, jnp.float32),
            pltpu.VMEM((local, n, rows, wide), jnp.float32),
            pltpu.VMEM((local, k, side, side), jnp.float32),
            pltpu.VMEM((2, rows, wide), jnp.float32),
            dma((local,)), dma(()), dma(()),
            dma(()), dma((local,)),
            dma(()), dma((2,)),
            dma(()), dma((2,)),
            *[pltpu.SemaphoreType.REGULAR] * 2,
        ],
        compiler_params=pltpu.CompilerParams(
            collective_id=0, has_side_effects=True, vmem_limit_bytes=VMEM_LIMIT),
    )(*[pltpu.with_memory_space_constraint(a, pltpu.HBM) for a in (gradients, momentum, weights)])


def finish_kernel(pieces, done_ref, new_ref, out_w, out_new, semaphores):
    step = done_ref.shape[0] // pieces
    copies = []
    for i in range(pieces):
        part = pl.ds(i * step, step)
        for source, target in ((done_ref, out_w), (new_ref, out_new)):
            copies.append(pltpu.make_async_copy(source.at[part], target.at[part], semaphores.at[len(copies)]))
    for copy in copies:
        copy.start()
    for copy in copies:
        copy.wait()


def finish(pieces, done, new_momentum):
    whole = jax.ShapeDtypeStruct(done.shape, jnp.float32)
    return pl.pallas_call(
        functools.partial(finish_kernel, pieces),
        out_shape=(whole, whole),
        in_specs=[pl.BlockSpec(memory_space=pltpu.VMEM)] * 2,
        out_specs=[pl.BlockSpec(memory_space=pl.ANY)] * 2,
        scratch_shapes=[pltpu.SemaphoreType.DMA((2 * pieces,))],
        compiler_params=pltpu.CompilerParams(vmem_limit_bytes=FINISH_LIMIT),
        cost_estimate=pl.CostEstimate(flops=2 * done.size, bytes_accessed=16 * done.size, transcendentals=0),
    )(done, new_momentum)


def on_device(n, k, gradients, momentum, weights):
    done, new_momentum = by_kernel(n, k, gradients, momentum, weights)
    return tuple(finish(2, done, new_momentum))


def solution(mesh):
    placed = P(None, "shard", "model")
    return jax.shard_map(
        functools.partial(on_device, mesh.shape["shard"], mesh.shape["model"]),
        mesh=mesh,
        in_specs=(placed, placed, placed),
        out_specs=(placed, placed),
        check_vma=False,
    )
```

```python
import functools

import jax
import jax.numpy as jnp
from jax import lax
from jax.experimental import pallas as pl
from jax.experimental.pallas import tpu as pltpu
from jax.sharding import PartitionSpec as P

ITERS = 4
VMEM_LIMIT = 40 * 1024 * 1024
FINISH_LIMIT = 16 * 1024 * 1024
MESH = pl.DeviceIdType.MESH
HIGHEST = lax.Precision.HIGHEST


hold_rate = 0.8
learn_rate = 1.0


def mm(a, b):
    return jnp.dot(a, b, precision=HIGHEST, preferred_element_type=jnp.float32)


def direction(gram):
    side = gram.shape[-1]
    row = lax.broadcasted_iota(jnp.int32, (side, side), 0)
    col = lax.broadcasted_iota(jnp.int32, (side, side), 1)
    diagonal = row == col
    squares = jnp.sum(jnp.where(diagonal, gram, 0.0), axis=(0, 1), keepdims=True)
    scale = lax.rsqrt(squares + 1e-06)
    a = gram * scale * scale
    q = jnp.where(diagonal, jnp.broadcast_to(scale, gram.shape), 0.0)
    for step in range(ITERS):
        mixed = -4.775 * a + 2.0315 * mm(a, a)
        if step == 0:
            q_next = 3.4445 * q + mixed * scale
        else:
            q_next = 3.4445 * q + mm(mixed, q)
        if step < ITERS - 1:
            half = 3.4445 * a + mm(mixed, a)
            a = 3.4445 * half + mm(mixed, half)
        q = q_next
    return q


def partner(me, off, n):
    if n & (n - 1):
        return lax.rem(me + off, n)
    for bit in range(n.bit_length() - 1):
        if (off >> bit) & 1:
            me = me + (1 - 2 * ((me // (1 << bit)) % 2)) * (1 << bit)
    return me


def partners(me, n):
    offs = range(n - 1, 0, -1)
    if n & (n - 1) or n < 8:
        return [(off, partner(me, off, n)) for off in offs]
    high, next_high = me // (n // 2), me // (n // 4) % 2
    inner = lax.rem(high + next_high, 2)
    found = []
    for off in offs:
        if off < n // 2:
            found.append((off, partner(me, off, n)))
        else:
            other = off ^ (n // 4)
            found.append((off + inner * (other - off),
                          partner(me, off, n) + inner * (partner(me, other, n) - partner(me, off, n))))
    return found


def across(me, n, upper):
    if n & (n - 1) or n < 8:
        return []
    quarter = n // 4
    shift = lax.rem(me // quarter + upper, 2) * quarter
    start = me // (2 * quarter) * -2 * quarter + (2 * quarter)
    return [(off + shift, start + upper * quarter + inner_place(me, off, quarter))
            for off in range(3 * quarter - 1, 2 * quarter - 1, -1)]


def inner_place(me, off, quarter):
    return partner(lax.rem(me, quarter), off % quarter, quarter)


def within(me, n):
    top = n - 1 if n & (n - 1) or n < 8 else n // 2 - 1
    return [(off, partner(me, off, n)) for off in range(top, 0, -1)]


def exchange_kernel(n, k, g_ref, m_ref, w_ref, done_ref, new_ref, pair, held, weight, result, grams, first,
                    l_pair, l_weight, l_first, f_send, f_recv, g_send, g_recv, b_send, b_recv, near, go):
    me = lax.axis_index("shard")
    col = lax.axis_index("model")
    local, _, rows, wide = held.shape
    side = n * rows
    early = n >= 8 and n & (n - 1) == 0
    middle = jnp.logical_and(me >= n // 2 - 2, me <= n // 2 + 1)
    lower = jnp.logical_and(middle, me < n // 2)
    hub = me == 0
    across_off, opposite_off = n - 1, n - 2
    opposite = partner(me, opposite_off, n)
    late = lax.rem(col, 2) == 1
    prompt = jnp.logical_and(middle, jnp.logical_not(late))

    def chunk(j):
        return pl.ds(j * n, n)

    def load_grad(j):
        return pltpu.make_async_copy(g_ref.at[chunk(j)], pair.at[j, 1], l_pair.at[j])

    def load_moved(j):
        return pltpu.make_async_copy(m_ref.at[chunk(j)], pair.at[j, 0], l_pair.at[j])

    def load_first(i, ref):
        return pltpu.make_async_copy(ref.at[opposite], first.at[i], l_first)

    def load_weight():
        return pltpu.make_async_copy(w_ref, weight, l_weight)

    def forward(j, off, to, source=None):
        return pltpu.make_async_remote_copy(
            src_ref=new_ref.at[j * n + to] if source is None else source, dst_ref=held.at[j, me],
            send_sem=f_send, recv_sem=f_recv.at[j],
            device_id={"shard": to}, device_id_type=MESH)

    def share(j, off):
        return pltpu.make_async_remote_copy(
            src_ref=grams.at[j, col], dst_ref=grams.at[j, col],
            send_sem=g_send, recv_sem=g_recv.at[lax.rem(j, 2)],
            device_id={"model": partner(col, off, k)}, device_id_type=MESH)

    def backward(j, off, to):
        return pltpu.make_async_remote_copy(
            src_ref=result.at[j, to], dst_ref=done_ref.at[j * n + me],
            send_sem=b_send, recv_sem=b_recv.at[j // max(local - 1, 1)],
            device_id={"shard": to}, device_id_type=MESH)

    def drain(ref, semaphore):
        pltpu.make_async_copy(ref, ref, semaphore).wait()

    def signal(semaphore, **to):
        pl.semaphore_signal(semaphore, inc=1, device_id=to, device_id_type=MESH)

    barrier = pltpu.get_barrier_semaphore()
    if early:
        load_first(0, m_ref).start()
        load_first(1, g_ref).start()

        @pl.when(middle)
        def _():
            signal(barrier, shard=opposite)

        @pl.when(lower)
        def _():
            signal(barrier, shard=partner(me, 1, n))

        @pl.when(jnp.logical_not(hub))
        def _():
            signal(barrier, shard=0)

        @pl.when(hub)
        def _():
            for off in range(1, k):
                signal(barrier, model=partner(col, off, k))
            for to in range(1, n):
                if not n // 2 - 2 <= to <= n // 2 + 1:
                    signal(barrier, shard=to)
    else:
        for off in range(n - 1, 0, -1):
            signal(barrier, shard=partner(me, off, n))
        for off in range(1, k):
            signal(barrier, model=partner(col, off, k))

    @pl.loop(0, local)
    def _(j):
        load_moved(j).start()
        load_grad(j).start()

    def step(j):
        drain(pair.at[j], l_pair.at[j])
        new_ref[chunk(j)] = hold_rate * pair[j, 0] + pair[j, 1]

    def send(j):
        for off, to in partners(me, n):
            if early:
                @pl.when(jnp.logical_not(jnp.logical_and(middle, off >= n - 2)))
                def _():
                    forward(j, off, to).start()
            else:
                forward(j, off, to).start()

    if early:
        drain(first, l_first)
        first[0] = hold_rate * first[0] + first[1]
        pl.semaphore_wait(barrier, jnp.where(hub, n + k - 2, jnp.where(lower, 2, 1)))

        @pl.when(middle)
        def _():
            forward(0, opposite_off, opposite, first.at[0]).start()

        @pl.when(lower)
        def _():
            signal(near, shard=partner(me, 1, n))
            signal(near, shard=opposite)

        @pl.loop(1, local)
        def _(j):
            step(j)

            @pl.when(jnp.logical_and(middle, jnp.logical_or(jnp.logical_not(late), j < local - 1)))
            def _():
                forward(j, opposite_off, opposite).start()

        step(0)

        @pl.when(middle)
        def _():
            pl.semaphore_wait(near, 1)

        @pl.when(prompt)
        def _():
            @pl.loop(0, local)
            def _(j):
                forward(j, across_off, partner(me, across_off, n)).start()
    else:
        step(0)
        pl.semaphore_wait(barrier, n + k - 2)

        @pl.loop(1, local)
        def _(j):
            step(j)

    if early:
        @pl.when(hub)
        def _():
            for off in range(1, k):
                signal(go, model=partner(col, off, k))
            pl.semaphore_wait(go, k - 1)
            for to in range(n - 1, 0, -1):
                signal(go, shard=to)

        @pl.when(jnp.logical_not(hub))
        def _():
            pl.semaphore_wait(go, 1)

    if early:
        @pl.when(jnp.logical_and(middle, late))
        def _():
            @pl.loop(max(local - 1, 1), local)
            def _(j):
                forward(j, opposite_off, opposite).start()

            @pl.loop(0, local)
            def _(j):
                forward(j, across_off, partner(me, across_off, n)).start()

    @pl.loop(0, local)
    def _(j):
        send(j)

    load_weight().start()

    @pl.loop(0, local)
    def _(j):
        held[j, me] = new_ref[j * n + me]
        drain(held.at[j, pl.ds(0, n - 1)], f_recv.at[j])
        x = held[j].reshape(side, wide)
        grams[j, col] = lax.dot_general(
            x, x, (((1,), (1,)), ((), ())), precision=HIGHEST, preferred_element_type=jnp.float32)
        for off in range(1, k):
            share(j, off).start()
        drain(grams.at[j, pl.ds(0, k - 1)], g_recv.at[lax.rem(j, 2)])
        gram = grams[j, 0]
        for i in range(1, k):
            gram = gram + grams[j, i]
        result[j] = mm(direction(gram), x).reshape(n, rows, wide)
        for off, to in across(me, n, 0):
            backward(j, off, to).start()

        @pl.when(jnp.logical_or(j < local - 2, j == local - 1))
        def _():
            @pl.loop(jnp.where(j == local - 1, max(local - 2, 0), j), j + 1)
            def _(i):
                for off, to in across(me, n, 1):
                    backward(i, off, to).start()

        for off, to in within(me, n):
            backward(j, off, to).start()
        done_ref[j * n + me] = result[j, me]

    load_weight().wait()

    def subtract(j):
        done_ref[chunk(j)] = weight[chunk(j)] - learn_rate * done_ref[chunk(j)]

    before = max(local - 1, 1)
    drain(done_ref.at[pl.ds(0, before * (n - 1))], b_recv.at[0])

    @pl.loop(0, before)
    def _(j):
        subtract(j)

    if before < local:
        drain(done_ref.at[pl.ds(0, n - 1)], b_recv.at[1])
        subtract(before)

    drain(new_ref.at[pl.ds(0, local * (n - 1))], f_send)
    drain(grams.at[:, pl.ds(0, k - 1)], g_send)
    drain(new_ref.at[pl.ds(0, local * (n - 1))], b_send)


def by_kernel(n, k, gradients, momentum, weights):
    mats, rows, wide = gradients.shape
    local = mats // n
    side = n * rows
    dma = pltpu.SemaphoreType.DMA
    whole = jax.ShapeDtypeStruct(gradients.shape, jnp.float32)
    return pl.pallas_call(
        functools.partial(exchange_kernel, n, k),
        out_shape=(whole, whole),
        in_specs=[pl.BlockSpec(memory_space=pltpu.HBM)] * 3,
        out_specs=[pl.BlockSpec(memory_space=pltpu.VMEM)] * 2,
        scratch_shapes=[
            pltpu.VMEM((local, 2, n, rows, wide), jnp.float32),
            pltpu.VMEM((local, n, rows, wide), jnp.float32),
            pltpu.VMEM(gradients.shape, jnp.float32),
            pltpu.VMEM((local, n, rows, wide), jnp.float32),
            pltpu.VMEM((local, k, side, side), jnp.float32),
            pltpu.VMEM((2, rows, wide), jnp.float32),
            dma((local,)), dma(()), dma(()),
            dma(()), dma((local,)),
            dma(()), dma((2,)),
            dma(()), dma((2,)),
            *[pltpu.SemaphoreType.REGULAR] * 2,
        ],
        compiler_params=pltpu.CompilerParams(
            collective_id=0, has_side_effects=True, vmem_limit_bytes=VMEM_LIMIT),
    )(*[pltpu.with_memory_space_constraint(a, pltpu.HBM) for a in (gradients, momentum, weights)])


def finish_kernel(done_ref, new_ref, out_w, out_new, semaphores):
    put_new = pltpu.make_async_copy(new_ref, out_new, semaphores.at[0])
    put_w = pltpu.make_async_copy(done_ref, out_w, semaphores.at[1])
    put_new.start()
    put_w.start()
    put_new.wait()
    put_w.wait()


def finish(done, new_momentum):
    whole = jax.ShapeDtypeStruct(done.shape, jnp.float32)
    return pl.pallas_call(
        finish_kernel,
        out_shape=(whole, whole),
        in_specs=[pl.BlockSpec(memory_space=pltpu.VMEM)] * 2,
        out_specs=[pl.BlockSpec(memory_space=pl.ANY)] * 2,
        scratch_shapes=[pltpu.SemaphoreType.DMA((2,))],
        compiler_params=pltpu.CompilerParams(vmem_limit_bytes=FINISH_LIMIT),
        cost_estimate=pl.CostEstimate(flops=2 * done.size, bytes_accessed=16 * done.size, transcendentals=0),
    )(done, new_momentum)


def on_device(n, k, gradients, momentum, weights):
    done, new_momentum = by_kernel(n, k, gradients, momentum, weights)
    return tuple(finish(done, new_momentum))


def solution(mesh):
    placed = P(None, "shard", "model")
    return jax.shard_map(
        functools.partial(on_device, mesh.shape["shard"], mesh.shape["model"]),
        mesh=mesh,
        in_specs=(placed, placed, placed),
        out_specs=(placed, placed),
        check_vma=False,
    )
```

```python
import functools

import jax
import jax.numpy as jnp
from jax import lax
from jax.experimental import pallas as pl
from jax.experimental.pallas import tpu as pltpu
from jax.sharding import PartitionSpec as P

ITERS = 4
VMEM_LIMIT = 40 * 1024 * 1024
FINISH_LIMIT = 16 * 1024 * 1024
MESH = pl.DeviceIdType.MESH
HIGHEST = lax.Precision.HIGHEST


hold_rate = 0.8
learn_rate = 1.0


def mm(a, b):
    return jnp.dot(a, b, precision=HIGHEST, preferred_element_type=jnp.float32)


def direction(gram):
    side = gram.shape[-1]
    row = lax.broadcasted_iota(jnp.int32, (side, side), 0)
    col = lax.broadcasted_iota(jnp.int32, (side, side), 1)
    diagonal = row == col
    squares = jnp.sum(jnp.where(diagonal, gram, 0.0), axis=(0, 1), keepdims=True)
    scale = lax.rsqrt(squares + 1e-06)
    a = gram * scale * scale
    q = jnp.where(diagonal, jnp.broadcast_to(scale, gram.shape), 0.0)
    for step in range(ITERS):
        mixed = -4.775 * a + 2.0315 * mm(a, a)
        if step == 0:
            q_next = 3.4445 * q + mixed * scale
        else:
            q_next = 3.4445 * q + mm(mixed, q)
        if step < ITERS - 1:
            half = 3.4445 * a + mm(mixed, a)
            a = 3.4445 * half + mm(mixed, half)
        q = q_next
    return q


def partner(me, off, n):
    if n & (n - 1):
        return lax.rem(me + off, n)
    for bit in range(n.bit_length() - 1):
        if (off >> bit) & 1:
            me = me + (1 - 2 * ((me // (1 << bit)) % 2)) * (1 << bit)
    return me


def partners(me, n):
    offs = range(n - 1, 0, -1)
    if n & (n - 1) or n < 8:
        return [(off, partner(me, off, n)) for off in offs]
    high, next_high = me // (n // 2), me // (n // 4) % 2
    inner = lax.rem(high + next_high, 2)
    found = []
    for off in offs:
        if off < n // 2:
            found.append((off, partner(me, off, n)))
        else:
            other = off ^ (n // 4)
            found.append((off + inner * (other - off),
                          partner(me, off, n) + inner * (partner(me, other, n) - partner(me, off, n))))
    return found


def across(me, n, upper):
    if n & (n - 1) or n < 8:
        return []
    quarter = n // 4
    shift = lax.rem(me // quarter + upper, 2) * quarter
    start = me // (2 * quarter) * -2 * quarter + (2 * quarter)
    return [(off + shift, start + upper * quarter + inner_place(me, off, quarter))
            for off in range(3 * quarter - 1, 2 * quarter - 1, -1)]


def inner_place(me, off, quarter):
    return partner(lax.rem(me, quarter), off % quarter, quarter)


def within(me, n):
    top = n - 1 if n & (n - 1) or n < 8 else n // 2 - 1
    return [(off, partner(me, off, n)) for off in range(top, 0, -1)]


def exchange_kernel(n, k, g_ref, m_ref, w_ref, done_ref, new_ref, pair, held, weight, result, grams, first,
                    l_pair, l_weight, l_first, f_send, f_recv, g_send, g_recv, b_send, b_recv, near, go):
    me = lax.axis_index("shard")
    col = lax.axis_index("model")
    local, _, rows, wide = held.shape
    side = n * rows
    early = n >= 8 and n & (n - 1) == 0
    middle = jnp.logical_and(me >= n // 2 - 2, me <= n // 2 + 1)
    lower = jnp.logical_and(middle, me < n // 2)
    hub = me == 0
    across_off, opposite_off = n - 1, n - 2
    opposite = partner(me, opposite_off, n)
    late = lax.rem(col, 2) == 1
    prompt = jnp.logical_and(middle, jnp.logical_not(late))

    def chunk(j):
        return pl.ds(j * n, n)

    def load_grad(j):
        return pltpu.make_async_copy(g_ref.at[chunk(j)], pair.at[j, 1], l_pair.at[j])

    def load_moved(j):
        return pltpu.make_async_copy(m_ref.at[chunk(j)], pair.at[j, 0], l_pair.at[j])

    def load_first(i, ref):
        return pltpu.make_async_copy(ref.at[opposite], first.at[i], l_first)

    def load_weight():
        return pltpu.make_async_copy(w_ref, weight, l_weight)

    def forward(j, off, to, source=None):
        return pltpu.make_async_remote_copy(
            src_ref=new_ref.at[j * n + to] if source is None else source, dst_ref=held.at[j, me],
            send_sem=f_send, recv_sem=f_recv.at[j],
            device_id={"shard": to}, device_id_type=MESH)

    def share(j, off):
        return pltpu.make_async_remote_copy(
            src_ref=grams.at[j, col], dst_ref=grams.at[j, col],
            send_sem=g_send, recv_sem=g_recv.at[lax.rem(j, 2)],
            device_id={"model": partner(col, off, k)}, device_id_type=MESH)

    def backward(j, off, to):
        return pltpu.make_async_remote_copy(
            src_ref=result.at[j, to], dst_ref=done_ref.at[j * n + me],
            send_sem=b_send, recv_sem=b_recv.at[j // max(local - 1, 1)],
            device_id={"shard": to}, device_id_type=MESH)

    def drain(ref, semaphore):
        pltpu.make_async_copy(ref, ref, semaphore).wait()

    def signal(semaphore, **to):
        pl.semaphore_signal(semaphore, inc=1, device_id=to, device_id_type=MESH)

    barrier = pltpu.get_barrier_semaphore()
    if early:
        load_first(0, m_ref).start()
        load_first(1, g_ref).start()

        @pl.when(middle)
        def _():
            signal(barrier, shard=opposite)

        @pl.when(lower)
        def _():
            signal(barrier, shard=partner(me, 1, n))

        @pl.when(jnp.logical_not(hub))
        def _():
            signal(barrier, shard=0)

        @pl.when(hub)
        def _():
            for off in range(1, k):
                signal(barrier, model=partner(col, off, k))
            for to in range(1, n):
                if not n // 2 - 2 <= to <= n // 2 + 1:
                    signal(barrier, shard=to)
    else:
        for off in range(n - 1, 0, -1):
            signal(barrier, shard=partner(me, off, n))
        for off in range(1, k):
            signal(barrier, model=partner(col, off, k))

    @pl.loop(0, local)
    def _(j):
        load_moved(j).start()
        load_grad(j).start()

    def step(j):
        drain(pair.at[j], l_pair.at[j])
        new_ref[chunk(j)] = hold_rate * pair[j, 0] + pair[j, 1]

    def send(j):
        for off, to in partners(me, n):
            if early:
                @pl.when(jnp.logical_not(jnp.logical_and(middle, off >= n - 2)))
                def _():
                    forward(j, off, to).start()
            else:
                forward(j, off, to).start()

    if early:
        drain(first, l_first)
        first[0] = hold_rate * first[0] + first[1]
        pl.semaphore_wait(barrier, jnp.where(hub, n + k - 2, jnp.where(lower, 2, 1)))

        @pl.when(middle)
        def _():
            forward(0, opposite_off, opposite, first.at[0]).start()

        @pl.when(lower)
        def _():
            signal(near, shard=partner(me, 1, n))
            signal(near, shard=opposite)

        @pl.loop(1, local)
        def _(j):
            step(j)

            @pl.when(jnp.logical_and(middle, jnp.logical_or(jnp.logical_not(late), j < local - 1)))
            def _():
                forward(j, opposite_off, opposite).start()

        step(0)

        @pl.when(middle)
        def _():
            pl.semaphore_wait(near, 1)

        @pl.when(prompt)
        def _():
            @pl.loop(0, local)
            def _(j):
                forward(j, across_off, partner(me, across_off, n)).start()
    else:
        step(0)
        pl.semaphore_wait(barrier, n + k - 2)

        @pl.loop(1, local)
        def _(j):
            step(j)

    if early:
        @pl.when(hub)
        def _():
            for off in range(1, k):
                signal(go, model=partner(col, off, k))
            pl.semaphore_wait(go, k - 1)
            for to in range(n - 1, 0, -1):
                signal(go, shard=to)

        @pl.when(jnp.logical_not(hub))
        def _():
            pl.semaphore_wait(go, 1)

    if early:
        @pl.when(jnp.logical_and(middle, late))
        def _():
            @pl.loop(max(local - 1, 1), local)
            def _(j):
                forward(j, opposite_off, opposite).start()

            @pl.loop(0, local)
            def _(j):
                forward(j, across_off, partner(me, across_off, n)).start()

    @pl.loop(0, local)
    def _(j):
        send(j)

    load_weight().start()

    @pl.loop(0, local)
    def _(j):
        held[j, me] = new_ref[j * n + me]
        drain(held.at[j, pl.ds(0, n - 1)], f_recv.at[j])
        x = held[j].reshape(side, wide)
        grams[j, col] = lax.dot_general(
            x, x, (((1,), (1,)), ((), ())), precision=HIGHEST, preferred_element_type=jnp.float32)
        for off in range(1, k):
            share(j, off).start()
        drain(grams.at[j, pl.ds(0, k - 1)], g_recv.at[lax.rem(j, 2)])
        gram = grams[j, 0]
        for i in range(1, k):
            gram = gram + grams[j, i]
        result[j] = mm(direction(gram), x).reshape(n, rows, wide)
        for off, to in across(me, n, 0):
            backward(j, off, to).start()

        @pl.when(j < local - 2)
        def _():
            for off, to in across(me, n, 1):
                backward(j, off, to).start()

        @pl.when(j == local - 1)
        def _():
            for off, to in across(me, n, 1):
                @pl.loop(max(local - 2, 0), local)
                def _(i):
                    backward(i, off, to).start()

        for off, to in within(me, n):
            backward(j, off, to).start()
        done_ref[j * n + me] = result[j, me]

    load_weight().wait()

    def subtract(j):
        done_ref[chunk(j)] = weight[chunk(j)] - learn_rate * done_ref[chunk(j)]

    before = max(local - 1, 1)
    drain(done_ref.at[pl.ds(0, before * (n - 1))], b_recv.at[0])

    @pl.loop(0, before)
    def _(j):
        subtract(j)

    if before < local:
        drain(done_ref.at[pl.ds(0, n - 1)], b_recv.at[1])
        subtract(before)

    drain(new_ref.at[pl.ds(0, local * (n - 1))], f_send)
    drain(grams.at[:, pl.ds(0, k - 1)], g_send)
    drain(new_ref.at[pl.ds(0, local * (n - 1))], b_send)


def by_kernel(n, k, gradients, momentum, weights):
    mats, rows, wide = gradients.shape
    local = mats // n
    side = n * rows
    dma = pltpu.SemaphoreType.DMA
    whole = jax.ShapeDtypeStruct(gradients.shape, jnp.float32)
    return pl.pallas_call(
        functools.partial(exchange_kernel, n, k),
        out_shape=(whole, whole),
        in_specs=[pl.BlockSpec(memory_space=pltpu.HBM)] * 3,
        out_specs=[pl.BlockSpec(memory_space=pltpu.VMEM)] * 2,
        scratch_shapes=[
            pltpu.VMEM((local, 2, n, rows, wide), jnp.float32),
            pltpu.VMEM((local, n, rows, wide), jnp.float32),
            pltpu.VMEM(gradients.shape, jnp.float32),
            pltpu.VMEM((local, n, rows, wide), jnp.float32),
            pltpu.VMEM((local, k, side, side), jnp.float32),
            pltpu.VMEM((2, rows, wide), jnp.float32),
            dma((local,)), dma(()), dma(()),
            dma(()), dma((local,)),
            dma(()), dma((2,)),
            dma(()), dma((2,)),
            *[pltpu.SemaphoreType.REGULAR] * 2,
        ],
        compiler_params=pltpu.CompilerParams(
            collective_id=0, has_side_effects=True, vmem_limit_bytes=VMEM_LIMIT),
    )(*[pltpu.with_memory_space_constraint(a, pltpu.HBM) for a in (gradients, momentum, weights)])


def finish_kernel(done_ref, new_ref, out_w, out_new, semaphores):
    put_new = pltpu.make_async_copy(new_ref, out_new, semaphores.at[0])
    put_w = pltpu.make_async_copy(done_ref, out_w, semaphores.at[1])
    put_new.start()
    put_w.start()
    put_new.wait()
    put_w.wait()


def finish(done, new_momentum):
    whole = jax.ShapeDtypeStruct(done.shape, jnp.float32)
    return pl.pallas_call(
        finish_kernel,
        out_shape=(whole, whole),
        in_specs=[pl.BlockSpec(memory_space=pltpu.VMEM)] * 2,
        out_specs=[pl.BlockSpec(memory_space=pl.ANY)] * 2,
        scratch_shapes=[pltpu.SemaphoreType.DMA((2,))],
        compiler_params=pltpu.CompilerParams(vmem_limit_bytes=FINISH_LIMIT),
        cost_estimate=pl.CostEstimate(flops=2 * done.size, bytes_accessed=16 * done.size, transcendentals=0),
    )(done, new_momentum)


def on_device(n, k, gradients, momentum, weights):
    done, new_momentum = by_kernel(n, k, gradients, momentum, weights)
    return tuple(finish(done, new_momentum))


def solution(mesh):
    placed = P(None, "shard", "model")
    return jax.shard_map(
        functools.partial(on_device, mesh.shape["shard"], mesh.shape["model"]),
        mesh=mesh,
        in_specs=(placed, placed, placed),
        out_specs=(placed, placed),
        check_vma=False,
    )
```
